32 devices in a mesh: rows: 16 (over z, y, x), cols: 2 (over core).
Axes of the slice: x: 2, y: 2, z: 4, core: 2. Of those that a mesh axis runs over, the one named last changes fastest.
Arguments:
- points: float32 [8, 4096], P(None, ('cols', 'rows')), may hold values from -6 to 6
- targets: float32 [4096], P(('cols', 'rows')), may hold values from -6 to 6
- noise: float32 [64, 4096], P(None, ('cols', 'rows')), may hold values from -6 to 6
- omega: float32 [8, 2048], P(None, 'rows'), may hold values from -12 to 12
- phase: float32 [2048], P('rows'), may hold values from -3.140625 to 3.140625
- weights: float32 [2048, 64], P('rows'), may hold values from -6 to 6
Outputs:
- posterior: float32 [64, 4096], P(None, ('cols', 'rows'))
- residual: float32 [64, 4096], P(None, ('cols', 'rows'))
The draws below stay inside these ranges and needn't reach their ends.
All inputs are finite; a program needn't handle non-finite values.
Results may differ from the reference program's by a relative error of at most 0.02.
Values may be sent and summed in bfloat16 or wider, within the bound.
A program may use at most 64 MiB of HBM per device.

```python
import math
import jax
import jax.numpy as jnp
from jax import lax

D_IN = 8
F = 2048
S = 64
ITERS = 2
N = 4096


def block_levels(own_key, extent, shards, least, high):
    def one(axis_at, blocks):
        draws = jax.random.uniform(jax.random.fold_in(jax.random.fold_in(own_key, 6), axis_at), (blocks,), jnp.float32, least / len(shards), high / len(shards))
        return jnp.repeat(jnp.exp(draws), extent[axis_at] // blocks).reshape((-1,) + (1,) * (len(extent) - axis_at - 1))

    gain = one(*shards[0])
    for cut in shards[1:]:
        gain = gain * one(*cut)
    return gain


def centred(stream_key, dims, spread, most, shards=(), held_as=jnp.bfloat16):
    factor_of = block_levels(stream_key, dims, shards, -0.22, 0.18) if shards else 1.0
    drawn = jax.random.normal(stream_key, dims, jnp.float32) * spread * factor_of
    return jnp.minimum(jnp.maximum(drawn, -most), most).astype(held_as)


def setup_inputs(seed: int = 0) -> dict:
    arg_keys = jax.random.split(jax.random.key(seed), 7)
    return {
        "points": centred(arg_keys[0], (D_IN, N), 1.0, 6.0, ((1, 32),), jnp.float32),
        "targets": centred(arg_keys[1], (N,), 1.0, 6.0, ((0, 32),), jnp.float32),
        "noise": centred(arg_keys[2], (S, N), 1.0, 6.0, ((1, 32),), jnp.float32),
        "omega": centred(arg_keys[3], (D_IN, F), 2.0, 12.0, ((1, 16),), jnp.float32),
        "phase": jnp.clip(jax.random.uniform(arg_keys[4], (F,), jnp.float32, -3.140625, 3.140625), -3.140625, 3.140625),
        "weights": centred(arg_keys[5], (F, S), 1.0, 6.0, ((0, 16),), jnp.float32),
    }


def kernel_block(left, right):
    cross = lax.dot_general(left, right, (((0,), (0,)), ((), ())), precision=lax.Precision.HIGHEST, preferred_element_type=jnp.float32)
    left_sq = lax.optimization_barrier(jnp.sum(left * left, 0))
    right_sq = lax.optimization_barrier(jnp.sum(right * right, 0))
    dist = left_sq[:, None] + right_sq[None, :] - 2.0 * cross
    return jnp.exp(-2.0 * dist).astype(jnp.bfloat16)

def apply_kernel(points, direction):
    width = math.gcd(N, 512)
    count = N // width
    low = direction.astype(jnp.bfloat16)
    blocks = points.reshape(D_IN, count, width).transpose(1, 0, 2)

    def one_block(block):
        return jnp.dot(low, kernel_block(points, block), preferred_element_type=jnp.float32)
    out = lax.map(one_block, blocks)
    return out.transpose(1, 0, 2).reshape(S, N)

def reference(points, targets, noise, omega, phase, weights):
    features = jnp.cos(jnp.dot(omega.T, points, precision=lax.Precision.HIGHEST, preferred_element_type=jnp.float32) + phase[:, None])
    prior = math.sqrt(2.0 / F) * jnp.dot(weights.T, features, precision=lax.Precision.HIGHEST, preferred_element_type=jnp.float32)
    rhs = targets[None, :] - prior - 0.5 * noise
    residual = rhs
    direction = rhs
    posterior = prior
    norm_now = lax.optimization_barrier(jnp.sum(residual * residual, 1))
    for step in range(ITERS):
        kernel_part = apply_kernel(points, direction)
        image = kernel_part + 0.25 * direction
        alpha = norm_now / lax.optimization_barrier(jnp.sum(direction * image, 1))
        posterior = posterior + alpha[:, None] * kernel_part
        residual = residual - alpha[:, None] * image
        if step + 1 < ITERS:
            norm_next = lax.optimization_barrier(jnp.sum(residual * residual, 1))
            direction = residual + (norm_next / norm_now)[:, None] * direction
            norm_now = norm_next
    return (posterior, residual)
```

```python
import functools
import math

import jax
import jax.numpy as jnp
from jax import lax
from jax.experimental import pallas as pl
from jax.experimental.pallas import tpu as pltpu
from jax.sharding import PartitionSpec as P

MESH = pl.DeviceIdType.MESH
LOG2E = math.log2(math.e)
COS = (
    0.9999999889,
    -19.73920447,
    64.93911593,
    -85.45011343,
    60.16742979,
    -25.96688461,
    6.527705963,
)
PTS, OMG, PHA, WTS, LOW, IMG, LOWF, IMGF, ST0, ST1, ST2 = range(11)
KINDS = 11


def loop(count, body):
    if count <= 32:
        for k in range(count):
            body(k)
    else:
        lax.fori_loop(0, count, lambda k, c: (body(k), c)[1], 0)


def split(x):
    high = x.astype(jnp.bfloat16).astype(jnp.float32)
    rest = x - high
    mid = rest.astype(jnp.bfloat16).astype(jnp.float32)
    return high, mid, rest - mid


def rows_of(x):
    high, mid, low = split(x)
    at = lax.broadcasted_iota(jnp.int32, (8, x.shape[1]), 0)
    return jnp.where(at == 0, high, jnp.where(at == 1, mid, jnp.where(at == 2, low, 0.0)))


def right_stack(x, seventh, eighth):
    high, mid, low = split(x)
    parts = (high, mid, low, high, mid, high, seventh, eighth)
    return jnp.concatenate(parts, 0).astype(jnp.bfloat16)


def cosine(turns):
    r = turns - jnp.floor(turns + 0.5)
    y = r * r
    out = COS[-1]
    for c in COS[-2::-1]:
        out = out * y + c
    return out


def nt(a, b):
    return lax.dot_general(a, b, (((1,), (1,)), ((), ())), preferred_element_type=jnp.float32)


def kernel(
    R, C, scale,
    points, targets, noise, omega, phase, weights,
    post_out, res_out,
    pts, omg, pha, wts, low, img, kern, st0, st1, st2, coef, ssem, rsem, slots,
):
    n = R * C
    me_r = lax.axis_index("rows")
    me_c = lax.axis_index("cols")
    me = me_c * R + me_r
    S = noise.shape[0]
    B = noise.shape[1]

    barrier = pltpu.get_barrier_semaphore()

    def other(k):
        j = lax.rem(me + k, n)
        return j, (lax.rem(j, R), j // R)

    def hello(k):
        pl.semaphore_signal(barrier, inc=1, device_id=other(k + 1)[1], device_id_type=MESH)

    loop(n - 1, hello)

    def send(buf, slot, kind, to):
        return pltpu.make_async_remote_copy(
            src_ref=buf.at[slot], dst_ref=buf.at[slot],
            send_sem=ssem.at[kind],
            recv_sem=slots.at[kind - LOW, lax.rem(slot, R)] if kind in (LOW, IMG) else rsem.at[kind],
            device_id=to, device_id_type=MESH,
        )

    def many(buf, count, kind):
        return pltpu.make_async_remote_copy(
            src_ref=buf.at[pl.ds(0, count)], dst_ref=buf.at[pl.ds(0, count)],
            send_sem=ssem.at[kind], recv_sem=rsem.at[kind],
            device_id=(me_r, me_c), device_id_type=MESH,
        )

    def arrived(buf, slot, kind):
        send(buf, slot, kind, (me_r, me_c)).wait_recv()

    mine = points[...]
    pts[me] = mine
    omg[me_r] = omega[...] * (0.5 / math.pi)
    pha[me_r] = phase[...].reshape(1, -1) * (0.5 / math.pi)
    wts[me_r] = weights[...].T.astype(jnp.bfloat16)
    high, mid, small = split(mine)
    own_sq = jnp.sum(mine * mine, 0, keepdims=True) * (-2.0 * LOG2E)
    ones = jnp.ones((8, B), jnp.float32)
    left = jnp.concatenate(
        (high, high, high, mid, mid, small, ones, rows_of(own_sq)), 0
    ).T.astype(jnp.bfloat16)

    pl.semaphore_wait(barrier, n - 1)

    def peer(k):
        return lax.rem(me_r + k + 1, R)

    def source(k):
        return lax.rem(me_r + R - 1 - k, R)

    def open_sends(k):
        to = (peer(k), me_c)
        send(omg, me_r, OMG, to).start()
        send(pha, me_r, PHA, to).start()
        send(wts, me_r, WTS, to).start()

    loop(R - 1, open_sends)

    def to_all(buf, kind):
        def one(k):
            j, to = other(k + 1)
            send(buf, me, kind, to).start()
        loop(n - 1, one)

    def from_all(buf, kind):
        many(buf, n - 1, kind).wait_recv()

    to_all(pts, PTS)

    for buf, kind in ((omg, OMG), (pha, PHA), (wts, WTS)):
        many(buf, R - 1, kind).wait_recv()

    width = omega.shape[1]
    group = 2 if width % 128 == 0 and R % 2 == 0 else 1

    def cat(buf, first, count):
        if count == 1:
            return buf[first]
        return jnp.concatenate([buf[first + i] for i in range(count)], 1)

    def features(g):
        o = cat(omg, g * group, group)
        p = cat(pha, g * group, group)
        right = right_stack(o, rows_of(p), jnp.zeros_like(o))
        turns = jnp.dot(left, right, preferred_element_type=jnp.float32)
        return nt(cat(wts, g * group, group), cosine(turns).astype(jnp.bfloat16))

    if R // group <= 32:
        prior = features(0)
        for g in range(1, R // group):
            prior = prior + features(g)
    else:
        prior = lax.fori_loop(
            0, R // group, lambda g, acc: acc + features(g), jnp.zeros((S, B), jnp.float32)
        )
    prior = scale * prior
    rhs = targets[...].reshape(1, -1) - prior - 0.5 * noise[...]

    low[me] = rhs.astype(jnp.bfloat16)

    def block_sends(buf, kind):
        loop(R - 1, lambda k: send(buf, me, kind, (peer(k), me_c)).start())

    def sibling(i):
        return lax.rem(me_c + i, C)

    def forward(buf, r, kind):
        for i in range(1, C):
            send(buf, me_c * R + r, kind + 2, (me_r, sibling(i))).start()

    block_sends(low, LOW)
    forward(low, me_r, LOW)

    eye = (
        lax.broadcasted_iota(jnp.int32, (S, 128), 0)
        == lax.broadcasted_iota(jnp.int32, (S, 128), 1)
    )

    def as_row(column):
        return jnp.sum(jnp.where(eye, column, 0.0), 0, keepdims=True)

    def as_column(row):
        return jnp.sum(jnp.where(eye, row, 0.0), 1, keepdims=True)

    rr_own = jnp.sum(rhs * rhs, 1, keepdims=True)
    st0[me] = as_row(rr_own)
    to_all(st0, ST0)

    from_all(pts, PTS)

    def kernel_chunk(g):
        b = cat(pts, g * C, C)
        sq = jnp.sum(b * b, 0, keepdims=True) * (-2.0 * LOG2E)
        right = right_stack(b * (4.0 * LOG2E), rows_of(sq), jnp.ones_like(b))
        power = jnp.dot(left, right, preferred_element_type=jnp.float32)
        kern[g] = jnp.exp2(power).astype(jnp.bfloat16)

    def relay(k):
        arrived(low, me_c * R + source(k), LOW)
        forward(low, source(k), LOW)
        kernel_chunk(k)

    loop(R - 1, relay)
    kernel_chunk(R - 1)

    def second_half(buf, kind):
        many(buf, R * (C - 1), kind + 2).wait_recv()

    second_half(low, LOW)

    def accumulate(block):
        if R <= 32:
            acc = nt(block(0), kern[0])
            for g in range(1, R):
                acc = acc + nt(block(g), kern[g])
            return acc
        return lax.fori_loop(
            0, R, lambda g, acc: acc + nt(block(g), kern[g]), jnp.zeros((S, B), jnp.float32)
        )

    part = accumulate(lambda g: cat(low, g * C, C))
    image = part + 0.25 * rhs
    share = jnp.sum(rhs * image, 1, keepdims=True)
    share = jnp.where(rr_own > 0.0, share / rr_own, 0.0)
    off = image - share * rhs
    img[me] = off.astype(jnp.bfloat16)
    block_sends(img, IMG)
    forward(img, me_r, IMG)
    st1[me] = jnp.concatenate(
        (
            as_row(share),
            as_row(jnp.sum(off * off, 1, keepdims=True)),
            as_row(jnp.sum(off * rhs, 1, keepdims=True)),
            jnp.zeros((1, 128), jnp.float32),
        ),
        0,
    )
    to_all(st1, ST1)
    from_all(st0, ST0)

    def relay_image(k):
        arrived(img, me_c * R + source(k), IMG)
        forward(img, source(k), IMG)

    loop(R - 1, relay_image)
    from_all(st1, ST1)
    norms = st0[:, 0, :]
    shares = st1[:, 0, :]
    squares = st1[:, 1, :]
    mixed = st1[:, 2, :]
    live = lax.broadcasted_iota(jnp.int32, (1, 128), 1) < S
    total = lambda x: jnp.sum(x, 0, keepdims=True)
    norm = total(norms)
    alpha = jnp.where(live, norm / total(shares * norms + mixed), 0.0)
    left_over = 1.0 - alpha * shares
    norm_next = total(
        left_over * left_over * norms
        + alpha * alpha * squares
        - 2.0 * alpha * left_over * mixed
    )
    beta = jnp.where(live, norm_next / norm, 0.0)
    coef[...] = beta + left_over
    alpha_c = as_column(alpha)
    beta_c = as_column(beta)
    residual = rhs - alpha_c * image
    direction = residual + beta_c * rhs
    posterior = prior + alpha_c * part

    second_half(img, IMG)

    def direction_block(j):
        c = as_column(coef[pl.ds(j, 1), :])
        return (c * low[j].astype(jnp.float32) - alpha_c * img[j].astype(jnp.float32)).astype(
            jnp.bfloat16
        )

    part = accumulate(
        lambda g: jnp.concatenate([direction_block(g * C + i) for i in range(C)], 1)
    )
    image = part + 0.25 * direction
    st2[me] = as_row(jnp.sum(direction * image, 1, keepdims=True))
    to_all(st2, ST2)

    for buf, kind in ((omg, OMG), (pha, PHA), (wts, WTS), (low, LOW), (img, IMG)):
        many(buf, R - 1, kind).wait_send()
    for buf, kind in ((low, LOWF), (img, IMGF)):
        many(buf, R * (C - 1), kind).wait_send()
    for buf, kind in ((pts, PTS), (st0, ST0), (st1, ST1)):
        many(buf, n - 1, kind).wait_send()

    from_all(st2, ST2)
    curve = total(st2[:, 0, :])
    alpha_c = as_column(jnp.where(live, norm_next / curve, 0.0))
    post_out[...] = posterior + alpha_c * part
    res_out[...] = residual - alpha_c * image
    many(st2, n - 1, ST2).wait_send()


def body(R, C, points, targets, noise, omega, phase, weights):
    n = R * C
    dim, B = points.shape
    width, S = weights.shape
    f32, bf16 = jnp.float32, jnp.bfloat16
    vmem = pl.BlockSpec(memory_space=pltpu.VMEM)
    return pl.pallas_call(
        functools.partial(kernel, R, C, math.sqrt(2.0 / (width * R))),
        out_shape=(
            jax.ShapeDtypeStruct(noise.shape, f32),
            jax.ShapeDtypeStruct(noise.shape, f32),
        ),
        in_specs=[vmem] * 6,
        out_specs=(vmem, vmem),
        scratch_shapes=[
            pltpu.VMEM((n, dim, B), f32),
            pltpu.VMEM((R, dim, width), f32),
            pltpu.VMEM((R, 1, width), f32),
            pltpu.VMEM((R, S, width), bf16),
            pltpu.VMEM((n, S, B), bf16),
            pltpu.VMEM((n, S, B), bf16),
            pltpu.VMEM((R, B, C * B), bf16),
            pltpu.VMEM((n, 1, 128), f32),
            pltpu.VMEM((n, 4, 128), f32),
            pltpu.VMEM((n, 1, 128), f32),
            pltpu.VMEM((n, 128), f32),
            pltpu.SemaphoreType.DMA((KINDS,)),
            pltpu.SemaphoreType.DMA((KINDS,)),
            pltpu.SemaphoreType.DMA((2, R)),
        ],
        compiler_params=pltpu.CompilerParams(collective_id=0, has_side_effects=True),
    )(points, targets, noise, omega, phase, weights)


def solution(mesh):
    return jax.shard_map(
        functools.partial(body, mesh.shape["rows"], mesh.shape["cols"]),
        mesh=mesh,
        in_specs=(
            P(None, ("cols", "rows")),
            P(("cols", "rows")),
            P(None, ("cols", "rows")),
            P(None, "rows"),
            P("rows"),
            P("rows", None),
        ),
        out_specs=(P(None, ("cols", "rows")), P(None, ("cols", "rows"))),
        check_vma=False,
    )
```

```python
import functools
import math

import jax
import jax.numpy as jnp
from jax import lax
from jax.experimental import pallas as pl
from jax.experimental.pallas import tpu as pltpu
from jax.sharding import PartitionSpec as P

MESH = pl.DeviceIdType.MESH
LOG2E = math.log2(math.e)
COS = (
    0.9999999889,
    -19.73920447,
    64.93911593,
    -85.45011343,
    60.16742979,
    -25.96688461,
    6.527705963,
)
PTS, OMG, PHA, WTS, LOW, IMG, LAST = range(7)
KINDS = 7


def loop(count, body):
    if count <= 32:
        for k in range(count):
            body(k)
    else:
        lax.fori_loop(0, count, lambda k, c: (body(k), c)[1], 0)


def split(x):
    high = x.astype(jnp.bfloat16).astype(jnp.float32)
    rest = x - high
    mid = rest.astype(jnp.bfloat16).astype(jnp.float32)
    return high, mid, rest - mid


def rows_of(x):
    high, mid, low = split(x)
    at = lax.broadcasted_iota(jnp.int32, (8, x.shape[1]), 0)
    return jnp.where(at == 0, high, jnp.where(at == 1, mid, jnp.where(at == 2, low, 0.0)))


def right_stack(x, seventh, eighth):
    high, mid, low = split(x)
    parts = (high, mid, low, high, mid, high, seventh, eighth)
    return jnp.concatenate(parts, 0).astype(jnp.bfloat16)


def cosine(turns):
    r = turns - jnp.floor(turns + 0.5)
    y = r * r
    out = COS[-1]
    for c in COS[-2::-1]:
        out = out * y + c
    return out


def nt(a, b):
    return lax.dot_general(a, b, (((1,), (1,)), ((), ())), preferred_element_type=jnp.float32)


def kernel(
    R, C, scale,
    points, targets, noise, omega, phase, weights,
    post_out, res_out,
    pts, omg, pha, wts, low, img, kern, last, coef, ssem, rsem, slots,
):
    n = R * C
    me_r = lax.axis_index("rows")
    me_c = lax.axis_index("cols")
    me = me_c * R + me_r
    S = noise.shape[0]
    B = noise.shape[1]

    barrier = pltpu.get_barrier_semaphore()

    def other(k):
        j = lax.rem(me + k, n)
        return j, (lax.rem(j, R), j // R)

    def hello(k):
        pl.semaphore_signal(barrier, inc=1, device_id=other(k + 1)[1], device_id_type=MESH)

    loop(n - 1, hello)

    A = 4 if R % 4 == 0 else 1
    Q = R // A
    plane = me_r // Q
    place = lax.rem(me_r, Q)
    NEAR, FAR, CORE = 0, 1, 2

    def send(buf, slot, kind, way, to):
        near = slots.at[kind, lax.rem(slot, R)]
        return pltpu.make_async_remote_copy(
            src_ref=buf.at[slot], dst_ref=buf.at[slot],
            send_sem=ssem.at[kind],
            recv_sem=near if way == NEAR else rsem.at[kind, way],
            device_id=to, device_id_type=MESH,
        )

    def many(buf, count, kind, way):
        return pltpu.make_async_remote_copy(
            src_ref=buf.at[pl.ds(0, count)], dst_ref=buf.at[pl.ds(0, count)],
            send_sem=ssem.at[kind], recv_sem=rsem.at[kind, way],
            device_id=(me_r, me_c), device_id_type=MESH,
        )

    def to_planes(buf, kind, base):
        def one(k):
            to = lax.rem(plane + k + 1, A) * Q + place
            send(buf, base + me_r, kind, NEAR, (to, me_c)).start()
        loop(A - 1, one)

    def to_places(buf, kind, base, r, way):
        def one(k):
            to = plane * Q + lax.rem(place + k + 1, Q)
            send(buf, base + r, kind, way, (to, me_c)).start()
        loop(Q - 1, one)

    def to_cores(buf, kind, r):
        for i in range(1, C):
            to = (me_r, lax.rem(me_c + i, C))
            send(buf, me_c * R + r, kind, CORE, to).start()

    def from_plane(k):
        return lax.rem(plane + A - 1 - k, A) * Q + place

    def arrived(buf, kind, base, r):
        send(buf, base + r, kind, NEAR, (me_r, me_c)).wait_recv()

    mine = points[...]
    pts[me] = mine
    omg[me_r] = omega[...] * (0.5 / math.pi)
    pha[me_r] = phase[...].reshape(1, -1) * (0.5 / math.pi)
    wts[me_r] = weights[...].astype(jnp.bfloat16)
    high, mid, small = split(mine)
    own_sq = jnp.sum(mine * mine, 0, keepdims=True) * (-2.0 * LOG2E)
    ones = jnp.ones((8, B), jnp.float32)
    left = jnp.concatenate(
        (high, high, high, mid, mid, small, ones, rows_of(own_sq)), 0
    ).T.astype(jnp.bfloat16)

    pl.semaphore_wait(barrier, n - 1)

    whole = me_c * R
    rows_data = ((omg, OMG), (pha, PHA), (wts, WTS))
    for buf, kind in rows_data:
        to_planes(buf, kind, 0)
    to_planes(pts, PTS, whole)
    for buf, kind in rows_data:
        to_places(buf, kind, 0, me_r, FAR)
    to_places(pts, PTS, whole, me_r, NEAR)
    to_cores(pts, PTS, me_r)

    def relay_rows(k):
        r = from_plane(k)
        for buf, kind in rows_data:
            arrived(buf, kind, 0, r)
            to_places(buf, kind, 0, r, FAR)

    def relay_points(k):
        r = from_plane(k)
        arrived(pts, PTS, whole, r)
        to_places(pts, PTS, whole, r, NEAR)
        to_cores(pts, PTS, r)

    loop(A - 1, relay_rows)
    loop(A - 1, relay_points)
    for buf, kind in rows_data:
        many(buf, R - A, kind, FAR).wait_recv()

    width = omega.shape[1]
    group = 2 if width % 128 == 0 and R % 2 == 0 else 1

    def cat(buf, first, count):
        if count == 1:
            return buf[first]
        return jnp.concatenate([buf[first + i] for i in range(count)], 1)

    def features(g):
        o = cat(omg, g * group, group)
        p = cat(pha, g * group, group)
        right = right_stack(o, rows_of(p), jnp.zeros_like(o))
        turns = jnp.dot(left, right, preferred_element_type=jnp.float32)
        return nt(cat(wts, g * group, group), cosine(turns).astype(jnp.bfloat16))

    if R // group <= 32:
        prior = features(0)
        for g in range(1, R // group):
            prior = prior + features(g)
    else:
        prior = lax.fori_loop(
            0, R // group, lambda g, acc: acc + features(g), jnp.zeros((S, B), jnp.float32)
        )
    prior = scale * prior
    rhs = targets[...].reshape(1, -1) - prior - 0.5 * noise[...]

    low[me] = rhs.astype(jnp.bfloat16)

    def far(k):
        p = lax.rem(plane + k // (Q - 1), A) if Q > 1 else 0
        return p * Q + lax.rem(place + 1 + lax.rem(k, max(Q - 1, 1)), Q)

    def open_gather(buf, kind):
        to_planes(buf, kind, whole)
        to_places(buf, kind, whole, me_r, NEAR)
        to_cores(buf, kind, me_r)

    def relay_planes(buf, kind, work):
        def one(k):
            r = from_plane(k)
            arrived(buf, kind, whole, r)
            to_places(buf, kind, whole, r, NEAR)
            to_cores(buf, kind, r)
            work(k)
        loop(A - 1, one)

    def relay_places(buf, kind, work):
        def one(k):
            r = far(k)
            arrived(buf, kind, whole, r)
            to_cores(buf, kind, r)
            work(k)
        loop(A * (Q - 1), one)

    def from_cores(buf, kind):
        many(buf, R * (C - 1), kind, CORE).wait_recv()

    open_gather(low, LOW)
    relay_places(pts, PTS, lambda k: None)

    eye = (
        lax.broadcasted_iota(jnp.int32, (S, 128), 0)
        == lax.broadcasted_iota(jnp.int32, (S, 128), 1)
    )

    def as_row(column):
        return jnp.sum(jnp.where(eye, column, 0.0), 0, keepdims=True)

    def as_column(row):
        return jnp.sum(jnp.where(eye, row, 0.0), 1, keepdims=True)

    rr_own = jnp.sum(rhs * rhs, 1, keepdims=True)
    from_cores(pts, PTS)

    def kernel_chunk(g):
        b = cat(pts, g * C, C)
        sq = jnp.sum(b * b, 0, keepdims=True) * (-2.0 * LOG2E)
        right = right_stack(b * (4.0 * LOG2E), rows_of(sq), jnp.ones_like(b))
        power = jnp.dot(left, right, preferred_element_type=jnp.float32)
        kern[g] = jnp.exp2(power).astype(jnp.bfloat16)

    relay_planes(low, LOW, kernel_chunk)
    relay_places(low, LOW, lambda k: kernel_chunk(A - 1 + k))
    kernel_chunk(R - 1)
    from_cores(low, LOW)

    def accumulate(block):
        if R <= 32:
            acc = nt(block(0), kern[0])
            for g in range(1, R):
                acc = acc + nt(block(g), kern[g])
            return acc
        return lax.fori_loop(
            0, R, lambda g, acc: acc + nt(block(g), kern[g]), jnp.zeros((S, B), jnp.float32)
        )

    part = accumulate(lambda g: cat(low, g * C, C))
    image = part + 0.25 * rhs
    share = jnp.sum(rhs * image, 1, keepdims=True)
    share = jnp.where(rr_own > 0.0, share / rr_own, 0.0)
    off = image - share * rhs
    img[me, :S] = off.astype(jnp.bfloat16)
    sums = (
        as_row(rr_own),
        as_row(share),
        as_row(jnp.sum(off * off, 1, keepdims=True)),
        as_row(jnp.sum(off * rhs, 1, keepdims=True)),
    )
    pieces = [split(row) for row in sums]
    blank = jnp.zeros((4, 128), jnp.float32)
    img[me, S:] = jnp.concatenate(
        [p[i] for i in range(3) for p in pieces] + [blank], 0
    ).astype(jnp.bfloat16)
    open_gather(img, IMG)
    relay_planes(img, IMG, lambda k: None)
    relay_places(img, IMG, lambda k: None)
    from_cores(img, IMG)

    tail = img[:, S:, :].astype(jnp.float32)
    norms, shares, squares, mixed = (
        tail[:, i, :] + tail[:, 4 + i, :] + tail[:, 8 + i, :] for i in range(4)
    )
    live = lax.broadcasted_iota(jnp.int32, (1, 128), 1) < S
    total = lambda x: jnp.sum(x, 0, keepdims=True)
    norm = total(norms)
    alpha = jnp.where(live, norm / total(shares * norms + mixed), 0.0)
    left_over = 1.0 - alpha * shares
    norm_next = total(
        left_over * left_over * norms
        + alpha * alpha * squares
        - 2.0 * alpha * left_over * mixed
    )
    beta = jnp.where(live, norm_next / norm, 0.0)
    coef[...] = beta + left_over
    alpha_c = as_column(alpha)
    beta_c = as_column(beta)
    residual = rhs - alpha_c * image
    direction = residual + beta_c * rhs
    posterior = prior + alpha_c * part

    def direction_block(j):
        c = as_column(coef[pl.ds(j, 1), :])
        return (c * low[j].astype(jnp.float32) - alpha_c * img[j, :S].astype(jnp.float32)).astype(
            jnp.bfloat16
        )

    part = accumulate(
        lambda g: jnp.concatenate([direction_block(g * C + i) for i in range(C)], 1)
    )
    image = part + 0.25 * direction
    last[me] = as_row(jnp.sum(direction * image, 1, keepdims=True))

    def finish(k):
        send(last, me, LAST, FAR, other(k + 1)[1]).start()

    loop(n - 1, finish)
    sent = (A - 1) + A * (Q - 1)
    for buf, kind in rows_data:
        many(buf, sent, kind, FAR).wait_send()
    for buf, kind in ((pts, PTS), (low, LOW), (img, IMG)):
        many(buf, sent + R * (C - 1), kind, FAR).wait_send()
    many(last, n - 1, LAST, FAR).wait_recv()
    curve = total(last[:, 0, :])
    alpha_c = as_column(jnp.where(live, norm_next / curve, 0.0))
    post_out[...] = posterior + alpha_c * part
    res_out[...] = residual - alpha_c * image
    many(last, n - 1, LAST, FAR).wait_send()


def body(R, C, points, targets, noise, omega, phase, weights):
    n = R * C
    dim, B = points.shape
    weights = weights.T
    S, width = weights.shape
    f32, bf16 = jnp.float32, jnp.bfloat16
    vmem = pl.BlockSpec(memory_space=pltpu.VMEM)
    return pl.pallas_call(
        functools.partial(kernel, R, C, math.sqrt(2.0 / (width * R))),
        out_shape=(
            jax.ShapeDtypeStruct(noise.shape, f32),
            jax.ShapeDtypeStruct(noise.shape, f32),
        ),
        in_specs=[vmem] * 6,
        out_specs=(vmem, vmem),
        scratch_shapes=[
            pltpu.VMEM((n, dim, B), f32),
            pltpu.VMEM((R, dim, width), f32),
            pltpu.VMEM((R, 1, width), f32),
            pltpu.VMEM((R, S, width), bf16),
            pltpu.VMEM((n, S, B), bf16),
            pltpu.VMEM((n, S + 16, B), bf16),
            pltpu.VMEM((R, B, C * B), bf16),
            pltpu.VMEM((n, 1, 128), f32),
            pltpu.VMEM((n, 128), f32),
            pltpu.SemaphoreType.DMA((KINDS,)),
            pltpu.SemaphoreType.DMA((KINDS, 3)),
            pltpu.SemaphoreType.DMA((KINDS, R)),
        ],
        compiler_params=pltpu.CompilerParams(collective_id=0, has_side_effects=True),
    )(points, targets, noise, omega, phase, weights)


def solution(mesh):
    return jax.shard_map(
        functools.partial(body, mesh.shape["rows"], mesh.shape["cols"]),
        mesh=mesh,
        in_specs=(
            P(None, ("cols", "rows")),
            P(("cols", "rows")),
            P(None, ("cols", "rows")),
            P(None, "rows"),
            P("rows"),
            P("rows", None),
        ),
        out_specs=(P(None, ("cols", "rows")), P(None, ("cols", "rows"))),
        check_vma=False,
    )
```

```python
import functools
import math

import jax
import jax.numpy as jnp
from jax import lax
from jax.experimental import pallas as pl
from jax.experimental.pallas import tpu as pltpu
from jax.sharding import PartitionSpec as P

MESH = pl.DeviceIdType.MESH
LOG2E = math.log2(math.e)
COS = (
    0.9999999889,
    -19.73920447,
    64.93911593,
    -85.45011343,
    60.16742979,
    -25.96688461,
    6.527705963,
)
PTS, OMG, PHA, WTS, LOW, IMG, LAST = range(7)
KINDS = 7


def loop(count, body):
    if count <= 32:
        for k in range(count):
            body(k)
    else:
        lax.fori_loop(0, count, lambda k, c: (body(k), c)[1], 0)


def split(x):
    high = x.astype(jnp.bfloat16).astype(jnp.float32)
    rest = x - high
    mid = rest.astype(jnp.bfloat16).astype(jnp.float32)
    return high, mid, rest - mid


def rows_of(x):
    high, mid, low = split(x)
    at = lax.broadcasted_iota(jnp.int32, (8, x.shape[1]), 0)
    return jnp.where(at == 0, high, jnp.where(at == 1, mid, jnp.where(at == 2, low, 0.0)))


def right_stack(x, seventh, eighth):
    high, mid, low = split(x)
    parts = (high, mid, low, high, mid, high, seventh, eighth)
    return jnp.concatenate(parts, 0).astype(jnp.bfloat16)


def cosine(turns):
    r = turns - jnp.floor(turns + 0.5)
    y = r * r
    out = COS[-1]
    for c in COS[-2::-1]:
        out = out * y + c
    return out


def nt(a, b):
    return lax.dot_general(a, b, (((1,), (1,)), ((), ())), preferred_element_type=jnp.float32)


def kernel(
    R, C, scale,
    points, targets, noise, omega, phase, weights,
    post_out, res_out,
    pts, omg, pha, wts, low, img, kern, last, coef, ssem, rsem, slots,
):
    n = R * C
    me_r = lax.axis_index("rows")
    me_c = lax.axis_index("cols")
    me = me_c * R + me_r
    S = noise.shape[0]
    B = noise.shape[1]

    barrier = pltpu.get_barrier_semaphore()

    def other(k):
        j = lax.rem(me + k, n)
        return j, (lax.rem(j, R), j // R)

    A = 4 if R % 4 == 0 else 1
    Q = R // A
    plane = me_r // Q
    place = lax.rem(me_r, Q)
    NEAR, FAR, CORE = 0, 1, 2

    def hello(r, c):
        pl.semaphore_signal(barrier, inc=1, device_id=(r, c), device_id_type=MESH)

    loop(A - 1, lambda k: hello(lax.rem(plane + k + 1, A) * Q + place, me_c))
    loop(Q - 1, lambda k: hello(plane * Q + lax.rem(place + k + 1, Q), me_c))
    loop(C - 1, lambda k: hello(me_r, lax.rem(me_c + k + 1, C)))

    def send(buf, slot, kind, way, to):
        near = slots.at[kind, lax.rem(slot, R)]
        return pltpu.make_async_remote_copy(
            src_ref=buf.at[slot], dst_ref=buf.at[slot],
            send_sem=ssem.at[kind],
            recv_sem=near if way == NEAR else rsem.at[kind, way],
            device_id=to, device_id_type=MESH,
        )

    def many(buf, count, kind, way):
        return pltpu.make_async_remote_copy(
            src_ref=buf.at[pl.ds(0, count)], dst_ref=buf.at[pl.ds(0, count)],
            send_sem=ssem.at[kind], recv_sem=rsem.at[kind, way],
            device_id=(me_r, me_c), device_id_type=MESH,
        )

    def to_planes(buf, kind, base):
        def one(k):
            to = lax.rem(plane + k + 1, A) * Q + place
            send(buf, base + me_r, kind, NEAR, (to, me_c)).start()
        loop(A - 1, one)

    def to_places(buf, kind, base, r, way):
        def one(k):
            to = plane * Q + lax.rem(place + k + 1, Q)
            send(buf, base + r, kind, way, (to, me_c)).start()
        loop(Q - 1, one)

    def to_cores(buf, kind, r):
        for i in range(1, C):
            to = (me_r, lax.rem(me_c + i, C))
            send(buf, me_c * R + r, kind, CORE, to).start()

    def from_plane(k):
        return lax.rem(plane + A - 1 - k, A) * Q + place

    def arrived(buf, kind, base, r):
        send(buf, base + r, kind, NEAR, (me_r, me_c)).wait_recv()

    mine = points[...]
    pts[me] = mine
    omg[me_r] = omega[...] * (0.5 / math.pi)
    pha[me_r] = phase[...].reshape(1, -1) * (0.5 / math.pi)
    wts[me_r] = weights[...].astype(jnp.bfloat16)
    high, mid, small = split(mine)
    own_sq = jnp.sum(mine * mine, 0, keepdims=True) * (-2.0 * LOG2E)
    ones = jnp.ones((8, B), jnp.float32)
    left = jnp.concatenate(
        (high, high, high, mid, mid, small, ones, rows_of(own_sq)), 0
    ).T.astype(jnp.bfloat16)

    pl.semaphore_wait(barrier, A + Q + C - 3)

    whole = me_c * R
    rows_data = ((omg, OMG), (pha, PHA), (wts, WTS))
    for buf, kind in rows_data:
        to_planes(buf, kind, 0)
    to_planes(pts, PTS, whole)
    for buf, kind in rows_data:
        to_places(buf, kind, 0, me_r, FAR)
    to_places(pts, PTS, whole, me_r, NEAR)
    to_cores(pts, PTS, me_r)

    def relay_rows(k):
        r = from_plane(k)
        for buf, kind in rows_data:
            arrived(buf, kind, 0, r)
            to_places(buf, kind, 0, r, FAR)

    def relay_points(k):
        r = from_plane(k)
        arrived(pts, PTS, whole, r)
        to_places(pts, PTS, whole, r, NEAR)
        to_cores(pts, PTS, r)

    loop(A - 1, relay_rows)
    loop(A - 1, relay_points)
    for buf, kind in rows_data:
        many(buf, R - A, kind, FAR).wait_recv()

    width = omega.shape[1]
    group = 2 if width % 128 == 0 and R % 2 == 0 else 1

    def cat(buf, first, count):
        if count == 1:
            return buf[first]
        return jnp.concatenate([buf[first + i] for i in range(count)], 1)

    def features(g):
        o = cat(omg, g * group, group)
        p = cat(pha, g * group, group)
        right = right_stack(o, rows_of(p), jnp.zeros_like(o))
        turns = jnp.dot(left, right, preferred_element_type=jnp.float32)
        return nt(cat(wts, g * group, group), cosine(turns).astype(jnp.bfloat16))

    if R // group <= 32:
        prior = features(0)
        for g in range(1, R // group):
            prior = prior + features(g)
    else:
        prior = lax.fori_loop(
            0, R // group, lambda g, acc: acc + features(g), jnp.zeros((S, B), jnp.float32)
        )
    prior = scale * prior
    rhs = targets[...].reshape(1, -1) - prior - 0.5 * noise[...]

    low[me] = rhs.astype(jnp.bfloat16)

    def far(k):
        p = lax.rem(plane + k // (Q - 1), A) if Q > 1 else 0
        return p * Q + lax.rem(place + 1 + lax.rem(k, max(Q - 1, 1)), Q)

    def open_gather(buf, kind):
        to_planes(buf, kind, whole)
        to_places(buf, kind, whole, me_r, NEAR)
        to_cores(buf, kind, me_r)

    def relay_planes(buf, kind, work):
        def one(k):
            r = from_plane(k)
            arrived(buf, kind, whole, r)
            to_places(buf, kind, whole, r, NEAR)
            to_cores(buf, kind, r)
            work(k)
        loop(A - 1, one)

    def relay_places(buf, kind, work, first=0, last=A * (Q - 1)):
        def one(k):
            r = far(first + k)
            arrived(buf, kind, whole, r)
            to_cores(buf, kind, r)
            work(k)
        loop(last - first, one)

    def from_cores(buf, kind):
        many(buf, R * (C - 1), kind, CORE).wait_recv()

    open_gather(low, LOW)
    idle = lambda k: None
    relay_places(pts, PTS, idle)

    eye = (
        lax.broadcasted_iota(jnp.int32, (S, 128), 0)
        == lax.broadcasted_iota(jnp.int32, (S, 128), 1)
    )

    def as_row(column):
        return jnp.sum(jnp.where(eye, column, 0.0), 0, keepdims=True)

    def as_column(row):
        return jnp.sum(jnp.where(eye, row, 0.0), 1, keepdims=True)

    rr_own = jnp.sum(rhs * rhs, 1, keepdims=True)
    from_cores(pts, PTS)

    def kernel_chunk(g):
        b = cat(pts, g * C, C)
        sq = jnp.sum(b * b, 0, keepdims=True) * (-2.0 * LOG2E)
        right = right_stack(b * (4.0 * LOG2E), rows_of(sq), jnp.ones_like(b))
        power = jnp.dot(left, right, preferred_element_type=jnp.float32)
        kern[g] = jnp.exp2(power).astype(jnp.bfloat16)

    head = R // 4
    each = R // 8
    done = head + (A - 1) * each
    loop(head, kernel_chunk)
    relay_planes(low, LOW, lambda k: loop(each, lambda i: kernel_chunk(head + k * each + i)))
    steps = A * (Q - 1)
    paired = min(R - done, steps - (Q - 1))
    relay_places(low, LOW, idle, 0, steps - paired)
    relay_places(low, LOW, lambda k: kernel_chunk(done + k), steps - paired, steps)
    loop(R - done - paired, lambda k: kernel_chunk(done + paired + k))
    from_cores(low, LOW)

    def accumulate(block):
        if R <= 32:
            acc = nt(block(0), kern[0])
            for g in range(1, R):
                acc = acc + nt(block(g), kern[g])
            return acc
        return lax.fori_loop(
            0, R, lambda g, acc: acc + nt(block(g), kern[g]), jnp.zeros((S, B), jnp.float32)
        )

    part = accumulate(lambda g: cat(low, g * C, C))
    image = part + 0.25 * rhs
    share = jnp.sum(rhs * image, 1, keepdims=True)
    share = jnp.where(rr_own > 0.0, share / rr_own, 0.0)
    off = image - share * rhs
    img[me, :S] = off.astype(jnp.bfloat16)
    sums = (
        as_row(rr_own),
        as_row(share),
        as_row(jnp.sum(off * off, 1, keepdims=True)),
        as_row(jnp.sum(off * rhs, 1, keepdims=True)),
    )
    pieces = [split(row) for row in sums]
    blank = jnp.zeros((4, 128), jnp.float32)
    img[me, S:] = jnp.concatenate(
        [p[i] for i in range(3) for p in pieces] + [blank], 0
    ).astype(jnp.bfloat16)
    open_gather(img, IMG)
    relay_planes(img, IMG, idle)
    relay_places(img, IMG, idle)
    from_cores(img, IMG)

    tail = img[:, S:, :].astype(jnp.float32)
    norms, shares, squares, mixed = (
        tail[:, i, :] + tail[:, 4 + i, :] + tail[:, 8 + i, :] for i in range(4)
    )
    live = lax.broadcasted_iota(jnp.int32, (1, 128), 1) < S
    total = lambda x: jnp.sum(x, 0, keepdims=True)
    norm = total(norms)
    alpha = jnp.where(live, norm / total(shares * norms + mixed), 0.0)
    left_over = 1.0 - alpha * shares
    norm_next = total(
        left_over * left_over * norms
        + alpha * alpha * squares
        - 2.0 * alpha * left_over * mixed
    )
    beta = jnp.where(live, norm_next / norm, 0.0)
    coef[...] = beta + left_over
    alpha_c = as_column(alpha)
    beta_c = as_column(beta)
    residual = rhs - alpha_c * image
    direction = residual + beta_c * rhs
    posterior = prior + alpha_c * part

    def direction_block(j):
        c = as_column(coef[pl.ds(j, 1), :])
        return (c * low[j].astype(jnp.float32) - alpha_c * img[j, :S].astype(jnp.float32)).astype(
            jnp.bfloat16
        )

    part = accumulate(
        lambda g: jnp.concatenate([direction_block(g * C + i) for i in range(C)], 1)
    )
    image = part + 0.25 * direction
    last[me] = as_row(jnp.sum(direction * image, 1, keepdims=True))

    def finish(k):
        send(last, me, LAST, FAR, other(k + 1)[1]).start()

    loop(n - 1, finish)
    sent = (A - 1) + A * (Q - 1)
    for buf, kind in rows_data:
        many(buf, sent, kind, FAR).wait_send()
    for buf, kind in ((pts, PTS), (low, LOW), (img, IMG)):
        many(buf, sent + R * (C - 1), kind, FAR).wait_send()
    many(last, n - 1, LAST, FAR).wait_recv()
    curve = total(last[:, 0, :])
    alpha_c = as_column(jnp.where(live, norm_next / curve, 0.0))
    post_out[...] = posterior + alpha_c * part
    res_out[...] = residual - alpha_c * image
    many(last, n - 1, LAST, FAR).wait_send()


def body(R, C, points, targets, noise, omega, phase, weights):
    n = R * C
    dim, B = points.shape
    weights = weights.T
    S, width = weights.shape
    f32, bf16 = jnp.float32, jnp.bfloat16
    vmem = pl.BlockSpec(memory_space=pltpu.VMEM)
    return pl.pallas_call(
        functools.partial(kernel, R, C, math.sqrt(2.0 / (width * R))),
        out_shape=(
            jax.ShapeDtypeStruct(noise.shape, f32),
            jax.ShapeDtypeStruct(noise.shape, f32),
        ),
        in_specs=[vmem] * 6,
        out_specs=(vmem, vmem),
        scratch_shapes=[
            pltpu.VMEM((n, dim, B), f32),
            pltpu.VMEM((R, dim, width), f32),
            pltpu.VMEM((R, 1, width), f32),
            pltpu.VMEM((R, S, width), bf16),
            pltpu.VMEM((n, S, B), bf16),
            pltpu.VMEM((n, S + 16, B), bf16),
            pltpu.VMEM((R, B, C * B), bf16),
            pltpu.VMEM((n, 1, 128), f32),
            pltpu.VMEM((n, 128), f32),
            pltpu.SemaphoreType.DMA((KINDS,)),
            pltpu.SemaphoreType.DMA((KINDS, 3)),
            pltpu.SemaphoreType.DMA((KINDS, R)),
        ],
        compiler_params=pltpu.CompilerParams(collective_id=0, has_side_effects=True),
    )(points, targets, noise, omega, phase, weights)


def solution(mesh):
    return jax.shard_map(
        functools.partial(body, mesh.shape["rows"], mesh.shape["cols"]),
        mesh=mesh,
        in_specs=(
            P(None, ("cols", "rows")),
            P(("cols", "rows")),
            P(None, ("cols", "rows")),
            P(None, "rows"),
            P("rows"),
            P("rows", None),
        ),
        out_specs=(P(None, ("cols", "rows")), P(None, ("cols", "rows"))),
        check_vma=False,
    )
```
